512 devices in a mesh: dp: 64 (over z, y), tensor: 8 (over x, core).
Axes of the slice: x: 4, y: 8, z: 8, core: 2. Of those that a mesh axis runs over, the one named last changes fastest.
Arguments:
- grads: bfloat16 [64, 256, 14336], P('dp', None, 'tensor'), may hold values from -6 to 6
- residual: float32 [64, 256, 14336], P('dp', None, 'tensor'), may hold values from -4 to 4
- q_prev: float32 [14336, 64], P('tensor'), may hold values from -6 to 6
Outputs:
- q_next: float32 [14336, 64], P('tensor')
- basis: float32 [256, 64], replicated
- new_residual: float32 [64, 256, 14336], P('dp', None, 'tensor')
The draws below stay inside these ranges and needn't reach their ends.
All inputs are finite; a program needn't handle non-finite values.
Results may differ from the reference program's by a relative error of at most 0.0003.
Values sent between devices are 32-bit elements; how exact they have to be, the bound alone decides.
No kernel may reach another device: no remote copies, remote signals or barrier semaphores. Data moves between devices by JAX's collectives and lax.ppermute only.
A program may use at most 64 MiB of HBM per device.

```python
import jax
import jax.numpy as jnp
from jax import lax

ROWS = 256
RANK = 64
COLS = 14336
N_DP = 64


def shard_levels(stream_key, dims, cuts, least, high):
    loudness = 1.0
    for position, blocks in cuts:
        draws = jax.random.uniform(jax.random.fold_in(jax.random.fold_in(stream_key, 6), position), (blocks,), jnp.float32, least / len(cuts), high / len(cuts))
        loudness = loudness * jnp.repeat(jnp.exp(draws), dims[position] // blocks).reshape((-1,) + (1,) * (len(dims) - 1 - position))
    return loudness


def normal_values(rng, shape, scale, bound, cuts=(), kind=jnp.bfloat16):
    values = jax.random.normal(rng, shape, jnp.float32) * scale
    if len(cuts) > 0:
        values = shard_levels(rng, shape, cuts, -0.22, 0.18) * values
    return jnp.clip(values, min=-bound, max=bound).astype(kind)


def setup_inputs(seed: int = 0) -> dict:
    seeds = jax.random.split(jax.random.key(seed), 4)
    return {
        "grads": normal_values(seeds[0], (N_DP, ROWS, COLS), 1.0, 6.0, ((0, 64), (2, 8))),
        "residual": normal_values(seeds[1], (N_DP, ROWS, COLS), 0.5, 4.0, ((0, 64), (2, 8)), jnp.float32),
        "q_prev": normal_values(seeds[2], (COLS, RANK), 1.0, 6.0, ((0, 8),), jnp.float32),
    }


def reference(grads, residual, q_prev):
    high = lax.Precision.HIGHEST
    merged = grads.astype(jnp.float32) + residual
    left = jnp.einsum('irc,ck->rk', merged, q_prev.astype(jnp.float32), precision=high) / N_DP
    gram = jnp.dot(left.T, left, precision=high)
    lower = jnp.linalg.cholesky(gram)
    basis = jax.scipy.linalg.solve_triangular(lower, left.T, lower=True).T
    q_next = jnp.einsum('irc,rk->ck', merged, basis, precision=high) / N_DP
    update = jnp.dot(basis, q_next.T, precision=high)
    new_residual = merged - update[None]
    return (q_next, basis, new_residual)
```

```python
import jax
import jax.numpy as jnp
from jax import lax
from jax.experimental import pallas as pl
from jax.experimental.pallas import tpu as pltpu
from jax.sharding import PartitionSpec as P

EVERY = ("dp", "tensor")
ROWS, RANK, COLS = 256, 64, 1792
N_DP, LANES = 64, 128
LINES = COLS // LANES
CHUNKS, WIDE = 7, 256
VMEM = pltpu.MemorySpace.VMEM
HBM = pltpu.MemorySpace.HBM
F32, BF16 = jnp.float32, jnp.bfloat16
NN = (((1,), (0,)), ((), ()))
NT = (((1,), (1,)), ((), ()))


def device(z, y, t):
    return (z * 8 + y) * 8 + t


NEAR = [[device(z, 2 * h + l, t) for l in range(2) for t in range(8)] for z in range(8) for h in range(4)]
FAR = [[device(z, 2 * h + l, t) for z in range(8) for h in range(4)] for l in range(2) for t in range(8)]


def exchange(x, groups):
    return lax.all_to_all(x, EVERY, 0, 0, axis_index_groups=groups, tiled=True)


def dot(a, b, dims):
    return lax.dot_general(a, b, dims, preferred_element_type=F32)


def exact(a, b, dims):
    return lax.dot_general(a, b, dims, precision=lax.Precision.HIGHEST, preferred_element_type=F32)


def halves(x):
    high = x.astype(BF16)
    return high, (x - high.astype(F32)).astype(BF16)


def thirds(x):
    high = x.astype(BF16)
    rest = x - high.astype(F32)
    mid = rest.astype(BF16)
    return high, mid, (rest - mid.astype(F32)).astype(BF16)


def project(grads, residual, right, out, high, low, merged, g_buf, r_buf, q_buf, sems):
    copies = []
    for n in range(CHUNKS):
        at = pl.ds(n * WIDE, WIDE)
        trio = [
            pltpu.make_async_copy(grads.at[:, at], g_buf.at[:, at], sems.at[0, n]),
            pltpu.make_async_copy(residual.at[:, at], r_buf.at[:, at], sems.at[1, n]),
            pltpu.make_async_copy(right.at[:, at], q_buf.at[:, at], sems.at[2, n]),
        ]
        for copy in trio:
            copy.start()
        copies.append(trio)
    total = jnp.zeros((RANK, ROWS), F32)
    for n in range(CHUNKS):
        at = pl.ds(n * WIDE, WIDE)
        for copy in copies[n]:
            copy.wait()
        m = g_buf[:, at].astype(F32) + r_buf[:, at]
        merged[:, at] = m
        m_high, m_low = halves(m)
        high[:, at] = m_high
        low[:, at] = m_low
        q_high, q_low = halves(q_buf[:, at])
        both = dot(jnp.concatenate([q_high, q_low], axis=0), m_high, NT)
        total += both[:RANK] + both[RANK:] + dot(q_high, m_low, NT)
    for n in range(16):
        i, j = n // 2, n % 2
        out[n] = total[8 * i : 8 * i + 8, LANES * j : LANES * (j + 1)]


def pass_on(parts, out):
    total = parts[0]
    for n in range(1, parts.shape[0]):
        total += parts[n]
    for n in range(out.shape[0]):
        out[n] = total


def left_of(parts):
    left = [jnp.concatenate([parts[2 * i], parts[2 * i + 1]], axis=1) for i in range(8)]
    return jnp.concatenate(left, axis=0) * (1.0 / N_DP)


def share(parts, high, low, out):
    left_high, left_low = halves(left_of(parts))
    stacked = jnp.concatenate([left_high, left_low], axis=0)
    for n in range(CHUNKS):
        at = pl.ds(n * WIDE, WIDE)
        m_high = high[:, at]
        both = dot(stacked, m_high, NN)
        mine = both[:RANK] + both[RANK:] + dot(left_high, low[:, at], NN)
        for i in range(8):
            for j in range(2):
                line = 2 * n + j
                out[pl.ds(8 * i * LINES + line, 8, stride=LINES), :] = mine[
                    8 * i : 8 * i + 8, LANES * j : LANES * (j + 1)
                ]


def factor(parts, basis, wide, whiten):
    left = left_of(parts)
    gram = exact(left, left, NT)
    rows = lax.broadcasted_iota(jnp.int32, (8, LANES), 0)
    row = lax.broadcasted_iota(jnp.int32, (RANK, RANK), 0)
    col = lax.broadcasted_iota(jnp.int32, (RANK, RANK), 1)
    both = jnp.concatenate([jnp.where(row == col, 1.0, 0.0).astype(F32), gram], axis=1)
    v = [both[8 * i : 8 * i + 8] for i in range(8)]
    scaled = []
    for p in range(8):
        b = [
            {i: jnp.broadcast_to(v[i][:, RANK + 8 * p + j : RANK + 8 * p + j + 1], (8, LANES)) for i in range(p, 8)}
            for j in range(8)
        ]
        pivots = b[0][p]
        for k in range(8):
            if k:
                pivots = jnp.where(rows == k, b[k][p], pivots)
            inverse = 1.0 / b[k][p][k : k + 1]
            heads = [b[j][p][k : k + 1] for j in range(8)]
            pivot_row = v[p][k : k + 1]
            for i in range(p, 8):
                c = b[k][i] * inverse
                if i == p:
                    c = jnp.where(rows > k, c, 0.0)
                v[i] = v[i] - c * pivot_row
                for j in range(k + 1, 8):
                    b[j][i] = b[j][i] - c * heads[j]
        scaled.append(v[p] / jnp.sqrt(pivots))
    s = jnp.concatenate(scaled, axis=0)[:, :RANK]
    b_t = exact(s, left, NN)
    basis[...] = b_t
    b_high, b_low = halves(b_t.T)
    wide[...] = jnp.concatenate([b_high, b_high, b_low], axis=1)
    s = s * (1.0 / N_DP)
    s_high, s_mid, s_low = thirds(s)
    whiten[...] = jnp.concatenate([s_high, s_high, s_mid, s_high, s_low, s_mid], axis=1)


def gather_sum(parts, out):
    four = parts[0:56]
    for n in range(1, 16):
        four += parts[56 * n : 56 * n + 56]
    one = four[0:14] + four[14:28] + four[28:42] + four[42:56]
    four = jnp.concatenate([one] * 4, axis=0)
    for n in range(16):
        out[56 * n : 56 * n + 56] = four


def finish(parts, wide, whiten, merged, q_out, out, o_buf, sems):
    copies = []
    for n in range(CHUNKS):
        at = pl.ds(n * WIDE, WIDE)
        p = jnp.concatenate(
            [
                jnp.concatenate(
                    [parts[pl.ds(8 * i * LINES + 2 * n + j, 8, stride=LINES), :] for i in range(8)], axis=0
                )
                for j in range(2)
            ],
            axis=1,
        )
        p_high, p_mid, p_low = thirds(p)
        stack = jnp.concatenate([p_high, p_mid, p_high, p_low, p_high, p_mid], axis=0)
        q = dot(whiten[...], stack, NN)
        q_out[:, at] = q
        q_high, q_low = halves(q)
        update = dot(wide[...], jnp.concatenate([q_high, q_low, q_high], axis=0), NN)
        o_buf[:, at] = merged[:, at] - update
        copy = pltpu.make_async_copy(o_buf.at[:, at], out.at[:, at], sems.at[n])
        copy.start()
        copies.append(copy)
    for copy in copies:
        copy.wait()


def spec(space):
    return pl.BlockSpec(memory_space=space)


def call(kernel, out, ins, outs, flops, scratch=(), limit=16 << 20):
    return pl.pallas_call(
        kernel,
        out_shape=out,
        in_specs=[spec(s) for s in ins],
        out_specs=jax.tree.map(spec, outs),
        scratch_shapes=list(scratch),
        cost_estimate=pl.CostEstimate(flops=flops, bytes_accessed=1 << 20, transcendentals=0),
        compiler_params=pltpu.CompilerParams(vmem_limit_bytes=limit),
    )


def shape(*dims, dtype=F32):
    return jax.ShapeDtypeStruct(dims, dtype)


def local(grads, residual, q_prev):
    sent, high, low, merged = call(
        project,
        (shape(16, 8, LANES), shape(ROWS, COLS, dtype=BF16), shape(ROWS, COLS, dtype=BF16), shape(ROWS, COLS)),
        (HBM,) * 3,
        (VMEM,) * 4,
        1 << 28,
        (
            pltpu.VMEM((ROWS, COLS), BF16),
            pltpu.VMEM((ROWS, COLS), F32),
            pltpu.VMEM((RANK, COLS), F32),
            pltpu.SemaphoreType.DMA((3, CHUNKS)),
        ),
    )(grads[0], residual[0], q_prev.T)
    parts = exchange(sent, NEAR)
    sent = call(pass_on, shape(32, 8, LANES), (VMEM,), VMEM, 1 << 15)(parts)
    parts = exchange(sent, FAR)
    sent = call(pass_on, shape(16, 8, LANES), (VMEM,), VMEM, 1 << 15)(parts)
    left = exchange(sent, NEAR)
    sent = call(share, shape(N_DP * LINES, LANES), (VMEM,) * 3, VMEM, 1 << 28)(left, high, low)
    parts = lax.all_to_all(sent.reshape(N_DP, 1, COLS), "dp", 0, 0, tiled=True)
    basis, wide, whiten = call(
        factor,
        (shape(RANK, ROWS), shape(ROWS, 3 * RANK, dtype=BF16), shape(RANK, 6 * RANK, dtype=BF16)),
        (VMEM,),
        (VMEM,) * 3,
        1 << 28,
    )(left)
    sent = call(gather_sum, shape(N_DP * LINES, LANES), (VMEM,), VMEM, 1 << 17)(parts.reshape(N_DP * LINES, LANES))
    parts = lax.all_to_all(sent.reshape(N_DP, 1, COLS), "dp", 0, 0, tiled=True)
    q_next, new_residual = call(
        finish,
        (shape(RANK, COLS), shape(ROWS, COLS)),
        (VMEM,) * 4,
        (VMEM, HBM),
        1 << 28,
        (pltpu.VMEM((ROWS, COLS), F32), pltpu.SemaphoreType.DMA((CHUNKS,))),
    )(parts.reshape(N_DP * LINES, LANES), wide, whiten, merged)
    return (q_next.T, basis.T, new_residual[None])


def solution(mesh):
    return jax.shard_map(
        local,
        mesh=mesh,
        in_specs=(P("dp", None, "tensor"), P("dp", None, "tensor"), P("tensor", None)),
        out_specs=(P("tensor", None), P(), P("dp", None, "tensor")),
        check_vma=False,
    )
```

```python
import jax
import jax.numpy as jnp
from jax import lax
from jax.experimental import pallas as pl
from jax.experimental.pallas import tpu as pltpu
from jax.sharding import PartitionSpec as P

EVERY = ("dp", "tensor")
ROWS, RANK, COLS = 256, 64, 1792
N_DP, LANES = 64, 128
LINES = COLS // LANES
CHUNKS, WIDE = 7, 256
CUTS = ((0, 512), (512, 512), (1024, 512), (1536, 256))
VMEM, HBM = pltpu.MemorySpace.VMEM, pltpu.MemorySpace.HBM
F32, BF16 = jnp.float32, jnp.bfloat16
NN = (((1,), (0,)), ((), ()))
NT = (((1,), (1,)), ((), ()))


def grouped(key):
    sets = {}
    for z in range(8):
        for y in range(8):
            for t in range(8):
                group, place = key(z, y, t)
                sets.setdefault(group, []).append((place, (z * 8 + y) * 8 + t))
    return [[device for _, device in sorted(members)] for _, members in sorted(sets.items())]


def turned(key):
    return grouped(lambda z, y, t: key(z, y, t) if t % 2 == 0 else key(y, z, t))


NEAR = grouped(lambda z, y, t: ((z, y // 2), (y % 2, t)))
FAR = grouped(lambda z, y, t: ((y % 2, t), (z, y // 2)))
LINE = turned(lambda z, y, t: ((t, y // 2), (z, y % 2)))
REST = turned(lambda z, y, t: ((t, z, y % 2), y // 2))


def exchange(x, groups):
    return lax.all_to_all(x, EVERY, 0, 0, axis_index_groups=groups, tiled=True)


def dot(a, b, dims):
    return lax.dot_general(a, b, dims, preferred_element_type=F32)


def exact(a, b, dims):
    return lax.dot_general(a, b, dims, precision=lax.Precision.HIGHEST, preferred_element_type=F32)


def halves(x):
    high = x.astype(BF16)
    return high, (x - high.astype(F32)).astype(BF16)


def thirds(x):
    high = x.astype(BF16)
    rest = x - high.astype(F32)
    mid = rest.astype(BF16)
    return high, mid, (rest - mid.astype(F32)).astype(BF16)


def project(grads, residual, right, out, high, low, merged, g_buf, r_buf, q_buf, sems):
    copies = []
    for n in range(CHUNKS):
        at = pl.ds(n * WIDE, WIDE)
        trio = [
            pltpu.make_async_copy(grads.at[:, at], g_buf.at[:, at], sems.at[0, n]),
            pltpu.make_async_copy(residual.at[:, at], r_buf.at[:, at], sems.at[1, n]),
            pltpu.make_async_copy(right.at[:, at], q_buf.at[:, at], sems.at[2, n]),
        ]
        for copy in trio:
            copy.start()
        copies.append(trio)
    total = jnp.zeros((RANK, ROWS), F32)
    for n in range(CHUNKS):
        at = pl.ds(n * WIDE, WIDE)
        for copy in copies[n]:
            copy.wait()
        m = g_buf[:, at].astype(F32) + r_buf[:, at]
        merged[:, at] = m
        m_high, m_low = halves(m)
        high[:, at] = m_high
        low[:, at] = m_low
        q_high, q_low = halves(q_buf[:, at])
        both = dot(jnp.concatenate([q_high, q_low], axis=0), m_high, NT)
        total += both[:RANK] + both[RANK:] + dot(q_high, m_low, NT)
    for n in range(16):
        i, j = n // 2, n % 2
        out[n] = total[8 * i : 8 * i + 8, LANES * j : LANES * (j + 1)]


def pass_on(parts, *refs):
    out = refs[-1]
    total = parts[0]
    for n in range(1, parts.shape[0]):
        total += parts[n]
    for n in range(out.shape[0]):
        out[n] = total


def left_of(parts):
    left = [jnp.concatenate([parts[2 * i], parts[2 * i + 1]], axis=1) for i in range(8)]
    return jnp.concatenate(left, axis=0) * (1.0 / N_DP)


def place(i, line):
    tile = i * LINES + line
    return tile // 7, pl.ds(8 * (tile % 7), 8)


def share(parts, high, low, out):
    left_high, left_low = halves(left_of(parts))
    stacked = jnp.concatenate([left_high, left_low], axis=0)
    for n in range(CHUNKS):
        at = pl.ds(n * WIDE, WIDE)
        both = dot(stacked, high[:, at], NN)
        mine = both[:RANK] + both[RANK:] + dot(left_high, low[:, at], NN)
        for i in range(8):
            for j in range(2):
                receiver, rows = place(i, 2 * n + j)
                out[receiver, rows, :] = mine[8 * i : 8 * i + 8, LANES * j : LANES * (j + 1)]


def factor(parts, _, basis, wide, whiten):
    left = left_of(parts)
    gram = exact(left, left, NT)
    rows = lax.broadcasted_iota(jnp.int32, (8, LANES), 0)
    row = lax.broadcasted_iota(jnp.int32, (RANK, RANK), 0)
    col = lax.broadcasted_iota(jnp.int32, (RANK, RANK), 1)
    both = jnp.concatenate([jnp.where(row == col, 1.0, 0.0).astype(F32), gram], axis=1)
    v = [both[8 * i : 8 * i + 8] for i in range(8)]
    scaled = []
    for p in range(8):
        b = [
            {i: jnp.broadcast_to(v[i][:, RANK + 8 * p + j : RANK + 8 * p + j + 1], (8, LANES)) for i in range(p, 8)}
            for j in range(8)
        ]
        pivots = b[0][p]
        for k in range(8):
            if k:
                pivots = jnp.where(rows == k, b[k][p], pivots)
            inverse = 1.0 / b[k][p][k : k + 1]
            heads = [b[j][p][k : k + 1] for j in range(8)]
            pivot_row = v[p][k : k + 1]
            for i in range(p, 8):
                c = b[k][i] * inverse
                if i == p:
                    c = jnp.where(rows > k, c, 0.0)
                v[i] = v[i] - c * pivot_row
                for j in range(k + 1, 8):
                    b[j][i] = b[j][i] - c * heads[j]
        scaled.append(v[p] / jnp.sqrt(pivots))
    s = jnp.concatenate(scaled, axis=0)[:, :RANK]
    b_t = exact(s, left, NN)
    basis[...] = b_t
    b_high, b_low = halves(b_t.T)
    wide[...] = jnp.concatenate([b_high, b_high, b_low], axis=1)
    s_high, s_mid, s_low = thirds(s * (1.0 / N_DP))
    whiten[...] = jnp.concatenate([s_high, s_high, s_mid, s_high, s_low, s_mid], axis=1)


def finish(parts, wide, whiten, merged, q_out, out, q_buf, q_cat, o_buf, sems):
    copies = []

    def put(source, target, start, width, sem):
        at = pl.ds(start, width)
        copy = pltpu.make_async_copy(source.at[:, at], target.at[:, at], sem)
        copy.start()
        copies.append(copy)

    for n, (start, width) in enumerate(CUTS):
        columns = []
        for line in range(start // LANES, (start + width) // LANES):
            tiles = []
            for i in range(8):
                sender, rows = place(i, line)
                tiles.append(parts[sender, rows, :])
            columns.append(jnp.concatenate(tiles, axis=0))
        p_high, p_mid, p_low = thirds(jnp.concatenate(columns, axis=1))
        q = dot(whiten[...], jnp.concatenate([p_high, p_mid, p_high, p_low, p_high, p_mid], axis=0), NN)
        q_buf[:, start : start + width] = q
        put(q_buf, q_out, start, width, sems.at[0, n])
        q_high, q_low = halves(q)
        q_cat[:, start : start + width] = jnp.concatenate([q_high, q_low, q_high], axis=0)
    for n, (start, width) in enumerate(CUTS):
        at = slice(start, start + width)
        o_buf[:, at] = merged[:, at] - dot(wide[...], q_cat[:, at], NN)
        put(o_buf, out, start, width, sems.at[1, n])
    for copy in copies:
        copy.wait()


def call(kernel, out, ins, outs, flops, scratch=()):
    return pl.pallas_call(
        kernel,
        out_shape=out,
        in_specs=[pl.BlockSpec(memory_space=s) for s in ins],
        out_specs=jax.tree.map(lambda s: pl.BlockSpec(memory_space=s), outs),
        scratch_shapes=list(scratch),
        cost_estimate=pl.CostEstimate(flops=flops, bytes_accessed=1 << 20, transcendentals=0),
        compiler_params=pltpu.CompilerParams(vmem_limit_bytes=16 << 20),
    )


def shape(*dims, dtype=F32):
    return jax.ShapeDtypeStruct(dims, dtype)


def local(grads, residual, q_prev):
    sent, high, low, merged = call(
        project,
        (shape(16, 8, LANES), shape(ROWS, COLS, dtype=BF16), shape(ROWS, COLS, dtype=BF16), shape(ROWS, COLS)),
        (HBM,) * 3,
        (VMEM,) * 4,
        1 << 28,
        (
            pltpu.VMEM((ROWS, COLS), BF16),
            pltpu.VMEM((ROWS, COLS), F32),
            pltpu.VMEM((RANK, COLS), F32),
            pltpu.SemaphoreType.DMA((3, CHUNKS)),
        ),
    )(*(pltpu.with_memory_space_constraint(x, HBM) for x in (grads[0], residual[0], q_prev.T)))
    parts = exchange(sent, NEAR)
    parts = exchange(call(pass_on, shape(32, 8, LANES), (VMEM,), VMEM, 1 << 15)(parts), FAR)
    left = exchange(call(pass_on, shape(16, 8, LANES), (VMEM,), VMEM, 1 << 15)(parts), NEAR)
    sent = call(share, shape(16, 56, LANES), (VMEM,) * 3, VMEM, 1 << 28)(left, high, low)
    first = exchange(sent, LINE)
    second = exchange(call(pass_on, shape(4, 56, LANES), (VMEM,), VMEM, 1 << 17)(first), REST)
    basis, wide, whiten = call(
        factor,
        (shape(RANK, ROWS), shape(ROWS, 3 * RANK, dtype=BF16), shape(RANK, 6 * RANK, dtype=BF16)),
        (VMEM, VMEM),
        (VMEM,) * 3,
        1 << 28,
    )(left, first)
    sent = call(pass_on, shape(16, 56, LANES), (VMEM, VMEM), VMEM, 1 << 17)(second, whiten)
    third = exchange(sent, LINE)
    q_next, new_residual = call(
        finish,
        (HBM((RANK, COLS), F32), HBM((ROWS, COLS), F32)),
        (VMEM,) * 4,
        (HBM, HBM),
        1 << 28,
        (
            pltpu.VMEM((RANK, COLS), F32),
            pltpu.VMEM((3 * RANK, COLS), BF16),
            pltpu.VMEM((ROWS, COLS), F32),
            pltpu.SemaphoreType.DMA((2, len(CUTS))),
        ),
    )(third, wide, whiten, merged)
    return (q_next.T, basis.T, new_residual[None])


def solution(mesh):
    return jax.shard_map(
        local,
        mesh=mesh,
        in_specs=(P("dp", None, "tensor"), P("dp", None, "tensor"), P("tensor", None)),
        out_specs=(P("tensor", None), P(), P("dp", None, "tensor")),
        check_vma=False,
    )
```

```python
import jax
import jax.numpy as jnp
from jax import lax
from jax.experimental import pallas as pl
from jax.experimental.pallas import tpu as pltpu
from jax.sharding import PartitionSpec as P


EVERY = ("dp", "tensor")
ROWS, RANK, COLS = 256, 64, 1792
N_DP, LANES = 64, 128
LINES = COLS // LANES
CHUNKS, WIDE, HALF = 7, 256, COLS // 2
CUTS = ((0, 512), (512, 512), (1024, 512), (1536, 256))
VMEM, HBM = pltpu.MemorySpace.VMEM, pltpu.MemorySpace.HBM
F32, BF16 = jnp.float32, jnp.bfloat16
NN = (((1,), (0,)), ((), ()))
NT = (((1,), (1,)), ((), ()))


def grouped(key):
    sets = {}
    for z in range(8):
        for y in range(8):
            for t in range(8):
                group, place = key(z, y, t)
                sets.setdefault(group, []).append((place, (z * 8 + y) * 8 + t))
    return [[device for _, device in sorted(members)] for _, members in sorted(sets.items())]


def turned(key):
    return grouped(lambda z, y, t: key(z, y, t) if t % 2 == 0 else key(y, z, t))


NEAR = grouped(lambda z, y, t: ((z, y // 2), (y % 2, t)))
FAR = grouped(lambda z, y, t: ((y % 2, t), (z, y // 2)))
ROW = turned(lambda z, y, t: ((t, y), z))
LINE = turned(lambda z, y, t: ((t, y // 2), (z, y % 2)))
PAIRS = turned(lambda z, y, t: ((t, z, y // 2), y % 2))
REST = turned(lambda z, y, t: ((t, z, y % 2), y // 2))


def exchange(x, groups):
    return lax.all_to_all(x, EVERY, 0, 0, axis_index_groups=groups, tiled=True)


def dot(a, b, dims):
    return lax.dot_general(a, b, dims, preferred_element_type=F32)


def exact(a, b, dims):
    return lax.dot_general(a, b, dims, precision=lax.Precision.HIGHEST, preferred_element_type=F32)


def halves(x):
    high = x.astype(BF16)
    return high, (x - high.astype(F32)).astype(BF16)


def thirds(x):
    high = x.astype(BF16)
    rest = x - high.astype(F32)
    mid = rest.astype(BF16)
    return high, mid, (rest - mid.astype(F32)).astype(BF16)


def kept():
    line = lax.axis_index("dp")
    return jnp.where(lax.axis_index("tensor") % 2 == 0, line % 2, line // 8 % 2)


def half_of(ref, n):
    return ref[:, pl.ds(pl.multiple_of(n * HALF, LANES), HALF)]


def project(grads, residual, right, out, outgoing, own, merged, g_buf, r_buf, q_buf, sems):
    copies = []
    for n in range(CHUNKS):
        at = pl.ds(n * WIDE, WIDE)
        trio = [
            pltpu.make_async_copy(grads.at[:, at], g_buf.at[:, at], sems.at[0, n]),
            pltpu.make_async_copy(residual.at[:, at], r_buf.at[:, at], sems.at[1, n]),
            pltpu.make_async_copy(right.at[:, at], q_buf.at[:, at], sems.at[2, n]),
        ]
        for copy in trio:
            copy.start()
        copies.append(trio)
    total = jnp.zeros((RANK, ROWS), F32)
    for n in range(CHUNKS):
        at = pl.ds(n * WIDE, WIDE)
        for copy in copies[n]:
            copy.wait()
        m = g_buf[:, at].astype(F32) + r_buf[:, at]
        merged[:, at] = m
        m_high, m_low = halves(m)
        q_high, q_low = halves(q_buf[:, at])
        both = dot(jnp.concatenate([q_high, q_low], axis=0), m_high, NT)
        total += both[:RANK] + both[RANK:] + dot(q_high, m_low, NT)
    for n in range(16):
        i, j = n // 2, n % 2
        out[n] = total[8 * i : 8 * i + 8, LANES * j : LANES * (j + 1)]
    outgoing[...] = half_of(merged, 1 - kept())
    own[...] = half_of(merged, kept())


def pass_on(parts, *refs):
    out = refs[-1]
    total = parts[0]
    for n in range(1, parts.shape[0]):
        total += parts[n]
    for n in range(out.shape[0]):
        out[n] = total


def left_of(parts):
    left = [jnp.concatenate([parts[2 * i], parts[2 * i + 1]], axis=1) for i in range(8)]
    return jnp.concatenate(left, axis=0) * (1.0 / N_DP)


def place(i, line):
    tile = i * LINES + line
    return tile // 7, pl.ds(8 * (tile % 7), 8)


def share(parts, own, incoming, out):
    high, low = halves(own[...] + incoming[...])
    left_high, left_low = halves(left_of(parts))
    stacked = jnp.concatenate([left_high, left_low], axis=0)
    both = dot(stacked, high, NN)
    mine = both[:RANK] + both[RANK:] + dot(left_high, low, NN)
    for i in range(8):
        for line in range(7):
            out[i, 8 * line : 8 * line + 8, :] = mine[8 * i : 8 * i + 8, LANES * line : LANES * (line + 1)]


def factor(parts, _, basis, wide, whiten):
    left = left_of(parts)
    gram = exact(left, left, NT)
    rows = lax.broadcasted_iota(jnp.int32, (8, LANES), 0)
    row = lax.broadcasted_iota(jnp.int32, (RANK, RANK), 0)
    col = lax.broadcasted_iota(jnp.int32, (RANK, RANK), 1)
    both = jnp.concatenate([jnp.where(row == col, 1.0, 0.0).astype(F32), gram], axis=1)
    v = [both[8 * i : 8 * i + 8] for i in range(8)]
    scaled = []
    for p in range(8):
        b = [
            {i: jnp.broadcast_to(v[i][:, RANK + 8 * p + j : RANK + 8 * p + j + 1], (8, LANES)) for i in range(p, 8)}
            for j in range(8)
        ]
        pivots = b[0][p]
        for k in range(8):
            if k:
                pivots = jnp.where(rows == k, b[k][p], pivots)
            inverse = 1.0 / b[k][p][k : k + 1]
            heads = [b[j][p][k : k + 1] for j in range(8)]
            pivot_row = v[p][k : k + 1]
            for i in range(p, 8):
                c = b[k][i] * inverse
                if i == p:
                    c = jnp.where(rows > k, c, 0.0)
                v[i] = v[i] - c * pivot_row
                for j in range(k + 1, 8):
                    b[j][i] = b[j][i] - c * heads[j]
        scaled.append(v[p] / jnp.sqrt(pivots))
    s = jnp.concatenate(scaled, axis=0)[:, :RANK]
    b_t = exact(s, left, NN)
    basis[...] = b_t
    b_high, b_low = halves(b_t.T)
    wide[...] = jnp.concatenate([b_high, b_high, b_low], axis=1)
    s_high, s_mid, s_low = thirds(s * (1.0 / N_DP))
    whiten[...] = jnp.concatenate([s_high, s_high, s_mid, s_high, s_low, s_mid], axis=1)


def finish(parts, wide, whiten, grads, residual, q_out, out, q_buf, q_cat, o_buf, sems):
    copies = []

    def put(source, target, start, width, sem):
        at = pl.ds(start, width)
        copy = pltpu.make_async_copy(source.at[:, at], target.at[:, at], sem)
        copy.start()
        copies.append(copy)

    for n, (start, width) in enumerate(CUTS):
        columns = []
        for line in range(start // LANES, (start + width) // LANES):
            tiles = []
            for i in range(8):
                sender, rows = place(i, line)
                tiles.append(parts[sender, rows, :])
            columns.append(jnp.concatenate(tiles, axis=0))
        p_high, p_mid, p_low = thirds(jnp.concatenate(columns, axis=1))
        q = dot(whiten[...], jnp.concatenate([p_high, p_mid, p_high, p_low, p_high, p_mid], axis=0), NN)
        q_buf[:, start : start + width] = q
        put(q_buf, q_out, start, width, sems.at[0, n])
        q_high, q_low = halves(q)
        q_cat[:, start : start + width] = jnp.concatenate([q_high, q_low, q_high], axis=0)
    for n, (start, width) in enumerate(CUTS):
        at = slice(start, start + width)
        o_buf[:, at] = grads[:, at].astype(F32) + residual[:, at] - dot(wide[...], q_cat[:, at], NN)
        put(o_buf, out, start, width, sems.at[1, n])
    for copy in copies:
        copy.wait()


def call(kernel, out, ins, outs, flops, scratch=()):
    return pl.pallas_call(
        kernel,
        out_shape=out,
        in_specs=[pl.BlockSpec(memory_space=s) for s in ins],
        out_specs=jax.tree.map(lambda s: pl.BlockSpec(memory_space=s), outs),
        scratch_shapes=list(scratch),
        cost_estimate=pl.CostEstimate(flops=flops, bytes_accessed=1 << 20, transcendentals=0),
        compiler_params=pltpu.CompilerParams(vmem_limit_bytes=16 << 20),
    )


def shape(*dims, dtype=F32):
    return jax.ShapeDtypeStruct(dims, dtype)


def local(grads, residual, q_prev):
    sent, outgoing, own = call(
        project,
        (shape(16, 8, LANES), shape(ROWS, HALF), shape(ROWS, HALF)),
        (HBM,) * 3,
        (VMEM,) * 3,
        1 << 28,
        (
            pltpu.VMEM((ROWS, COLS), F32),
            pltpu.VMEM((ROWS, COLS), BF16),
            pltpu.VMEM((ROWS, COLS), F32),
            pltpu.VMEM((RANK, COLS), F32),
            pltpu.SemaphoreType.DMA((3, CHUNKS)),
        ),
    )(*(pltpu.with_memory_space_constraint(x, HBM) for x in (grads[0], residual[0], q_prev.T)))
    parts = exchange(sent, NEAR)
    incoming = lax.ppermute(outgoing, EVERY, [(a, b) for two in PAIRS for a, b in (two, two[::-1])])
    parts = exchange(call(pass_on, shape(32, 8, LANES), (VMEM,), VMEM, 1 << 15)(parts), FAR)
    left = exchange(call(pass_on, shape(16, 8, LANES), (VMEM,), VMEM, 1 << 15)(parts), NEAR)
    sent = call(share, shape(8, 56, LANES), (VMEM,) * 3, VMEM, 1 << 28)(left, own, incoming)
    first = exchange(sent, ROW)
    second = exchange(call(pass_on, shape(4, 56, LANES), (VMEM,), VMEM, 1 << 17)(first), REST)
    basis, wide, whiten = call(
        factor,
        (shape(RANK, ROWS), shape(ROWS, 3 * RANK, dtype=BF16), shape(RANK, 6 * RANK, dtype=BF16)),
        (VMEM, VMEM),
        (VMEM,) * 3,
        1 << 28,
    )(left, first)
    sent = call(pass_on, shape(16, 56, LANES), (VMEM, VMEM), VMEM, 1 << 17)(second, whiten)
    third = exchange(sent, LINE)
    q_next, new_residual = call(
        finish,
        (HBM((RANK, COLS), F32), HBM((ROWS, COLS), F32)),
        (VMEM,) * 5,
        (HBM, HBM),
        1 << 28,
        (
            pltpu.VMEM((RANK, COLS), F32),
            pltpu.VMEM((3 * RANK, COLS), BF16),
            pltpu.VMEM((ROWS, COLS), F32),
            pltpu.SemaphoreType.DMA((2, len(CUTS))),
        ),
    )(third, wide, whiten, grads[0], residual[0])
    return (q_next.T, basis.T, new_residual[None])


def solution(mesh):
    return jax.shard_map(
        local,
        mesh=mesh,
        in_specs=(P("dp", None, "tensor"), P("dp", None, "tensor"), P("tensor", None)),
        out_specs=(P("tensor", None), P(), P("dp", None, "tensor")),
        check_vma=False,
    )
```

```python
import jax
import jax.numpy as jnp
from jax import lax
from jax.experimental import pallas as pl
from jax.experimental.pallas import tpu as pltpu
from jax.sharding import PartitionSpec as P


EVERY = ("dp", "tensor")
ROWS, RANK, COLS = 256, 64, 1792
N_DP, LANES = 64, 128
LINES = COLS // LANES
HALF = COLS // 2
READS = tuple((n * 256, 256) for n in range(6)) + ((1536, 128), (1664, 128))
CUTS = ((0, 512), (512, 512), (1024, 512), (1536, 256))
VMEM, HBM = pltpu.MemorySpace.VMEM, pltpu.MemorySpace.HBM
F32, BF16 = jnp.float32, jnp.bfloat16
NN = (((1,), (0,)), ((), ()))
NT = (((1,), (1,)), ((), ()))


def grouped(key):
    sets = {}
    for z in range(8):
        for y in range(8):
            for t in range(8):
                group, place = key(z, y, t)
                sets.setdefault(group, []).append((place, (z * 8 + y) * 8 + t))
    return [[device for _, device in sorted(members)] for _, members in sorted(sets.items())]


def turned(key):
    return grouped(lambda z, y, t: key(z, y, t) if t % 2 == 1 else key(y, z, t))


NEAR = grouped(lambda z, y, t: ((z, y // 2), (y % 2, t)))
FAR = grouped(lambda z, y, t: ((y % 2, t), (z, y // 2)))
ROW = turned(lambda z, y, t: ((t, y), z))
LINE = turned(lambda z, y, t: ((t, y // 2), (z, y % 2)))
PAIRS = turned(lambda z, y, t: ((t, z, y // 2), y % 2))
REST = turned(lambda z, y, t: ((t, z, y % 2), y // 2))


def exchange(x, groups):
    return lax.all_to_all(x, EVERY, 0, 0, axis_index_groups=groups, tiled=True)


def dot(a, b, dims):
    return lax.dot_general(a, b, dims, preferred_element_type=F32)


def exact(a, b, dims):
    return lax.dot_general(a, b, dims, precision=lax.Precision.HIGHEST, preferred_element_type=F32)


def halves(x):
    high = x.astype(BF16)
    return high, (x - high.astype(F32)).astype(BF16)


def thirds(x):
    high = x.astype(BF16)
    rest = x - high.astype(F32)
    mid = rest.astype(BF16)
    return high, mid, (rest - mid.astype(F32)).astype(BF16)


def kept():
    line = lax.axis_index("dp")
    return jnp.where(lax.axis_index("tensor") % 2 == 1, line % 2, line // 8 % 2)


def half_of(ref, n):
    return ref[:, pl.ds(pl.multiple_of(n * HALF, LANES), HALF)]


def project(grads, residual, right, out, outgoing, own, merged, g_buf, r_buf, q_buf, tiles, sems, sent):
    copies = []
    for n, (start, width) in enumerate(READS):
        at = pl.ds(start, width)
        trio = [
            pltpu.make_async_copy(grads.at[:, at], g_buf.at[:, at], sems.at[0, n]),
            pltpu.make_async_copy(residual.at[:, at], r_buf.at[:, at], sems.at[1, n]),
            pltpu.make_async_copy(right.at[:, at], q_buf.at[:, at], sems.at[2, n]),
        ]
        for copy in trio:
            copy.start()
        copies.append(trio)
    total = jnp.zeros((RANK, ROWS), F32)
    for n, (start, width) in enumerate(READS):
        at = pl.ds(start, width)
        for copy in copies[n]:
            copy.wait()
        m = g_buf[:, at].astype(F32) + r_buf[:, at]
        merged[:, at] = m
        m_high, m_low = halves(m)
        q_high, q_low = halves(q_buf[:, at])
        both = dot(jnp.concatenate([q_high, q_low], axis=0), m_high, NT)
        total += both[:RANK] + both[RANK:] + dot(q_high, m_low, NT)
    for n in range(16):
        i, j = n // 2, n % 2
        tiles[n] = total[8 * i : 8 * i + 8, LANES * j : LANES * (j + 1)]
    copy = pltpu.make_async_copy(tiles, out, sent)
    copy.start()
    outgoing[...] = half_of(merged, 1 - kept())
    own[...] = half_of(merged, kept())
    copy.wait()


def pass_on(parts, *refs):
    out = refs[-1]
    total = parts[0]
    for n in range(1, parts.shape[0]):
        total += parts[n]
    for n in range(out.shape[0]):
        out[n] = total


def left_of(parts):
    left = [jnp.concatenate([parts[2 * i], parts[2 * i + 1]], axis=1) for i in range(8)]
    return jnp.concatenate(left, axis=0) * (1.0 / N_DP)


def place(i, line):
    tile = i * LINES + line
    return tile // 7, pl.ds(8 * (tile % 7), 8)


def share(parts, own, incoming, out):
    high, low = halves(own[...] + incoming[...])
    left_high, left_low = halves(left_of(parts))
    stacked = jnp.concatenate([left_high, left_low], axis=0)
    both = dot(stacked, high, NN)
    mine = both[:RANK] + both[RANK:] + dot(left_high, low, NN)
    for i in range(8):
        for line in range(7):
            out[i, 8 * line : 8 * line + 8, :] = mine[8 * i : 8 * i + 8, LANES * line : LANES * (line + 1)]


def factor(parts, _, basis, wide, whiten):
    left = left_of(parts)
    gram = exact(left, left, NT)
    rows = lax.broadcasted_iota(jnp.int32, (8, LANES), 0)
    row = lax.broadcasted_iota(jnp.int32, (RANK, RANK), 0)
    col = lax.broadcasted_iota(jnp.int32, (RANK, RANK), 1)
    both = jnp.concatenate([jnp.where(row == col, 1.0, 0.0).astype(F32), gram], axis=1)
    v = [both[8 * i : 8 * i + 8] for i in range(8)]
    scaled = []
    for p in range(8):
        b = [
            {i: jnp.broadcast_to(v[i][:, RANK + 8 * p + j : RANK + 8 * p + j + 1], (8, LANES)) for i in range(p, 8)}
            for j in range(8)
        ]
        pivots = b[0][p]
        for k in range(8):
            if k:
                pivots = jnp.where(rows == k, b[k][p], pivots)
            inverse = 1.0 / b[k][p][k : k + 1]
            heads = [b[j][p][k : k + 1] for j in range(8)]
            pivot_row = v[p][k : k + 1]
            for i in range(p, 8):
                c = b[k][i] * inverse
                if i == p:
                    c = jnp.where(rows > k, c, 0.0)
                v[i] = v[i] - c * pivot_row
                for j in range(k + 1, 8):
                    b[j][i] = b[j][i] - c * heads[j]
        scaled.append(v[p] / jnp.sqrt(pivots))
    s = jnp.concatenate(scaled, axis=0)[:, :RANK]
    b_t = exact(s, left, NN)
    basis[...] = b_t
    b_high, b_low = halves(b_t.T)
    wide[...] = jnp.concatenate([b_high, b_high, b_low], axis=1)
    s_high, s_mid, s_low = thirds(s * (1.0 / N_DP))
    whiten[...] = jnp.concatenate([s_high, s_high, s_mid, s_high, s_low, s_mid], axis=1)


def finish(parts, wide, whiten, grads, residual, q_out, out, q_buf, q_cat, o_buf, sems):
    copies = []

    def put(source, target, start, width, sem):
        at = pl.ds(start, width)
        copy = pltpu.make_async_copy(source.at[:, at], target.at[:, at], sem)
        copy.start()
        copies.append(copy)

    for n, (start, width) in enumerate(CUTS):
        columns = []
        for line in range(start // LANES, (start + width) // LANES):
            tiles = []
            for i in range(8):
                sender, rows = place(i, line)
                tiles.append(parts[sender, rows, :])
            columns.append(jnp.concatenate(tiles, axis=0))
        p_high, p_mid, p_low = thirds(jnp.concatenate(columns, axis=1))
        q = dot(whiten[...], jnp.concatenate([p_high, p_mid, p_high, p_low, p_high, p_mid], axis=0), NN)
        q_buf[:, start : start + width] = q
        put(q_buf, q_out, start, width, sems.at[0, n])
        q_high, q_low = halves(q)
        q_cat[:, start : start + width] = jnp.concatenate([q_high, q_low, q_high], axis=0)
    for n, (start, width) in enumerate(CUTS):
        at = slice(start, start + width)
        o_buf[:, at] = grads[:, at].astype(F32) + residual[:, at] - dot(wide[...], q_cat[:, at], NN)
        put(o_buf, out, start, width, sems.at[1, n])
    for copy in copies:
        copy.wait()


def call(kernel, out, ins, outs, flops, scratch=()):
    return pl.pallas_call(
        kernel,
        out_shape=out,
        in_specs=[pl.BlockSpec(memory_space=s) for s in ins],
        out_specs=jax.tree.map(lambda s: pl.BlockSpec(memory_space=s), outs),
        scratch_shapes=list(scratch),
        cost_estimate=pl.CostEstimate(flops=flops, bytes_accessed=1 << 20, transcendentals=0),
        compiler_params=pltpu.CompilerParams(vmem_limit_bytes=16 << 20),
    )


def shape(*dims, dtype=F32):
    return jax.ShapeDtypeStruct(dims, dtype)


def local(grads, residual, q_prev):
    sent, outgoing, own = call(
        project,
        (HBM((16, 8, LANES), F32), shape(ROWS, HALF), shape(ROWS, HALF)),
        (HBM,) * 3,
        (HBM, VMEM, VMEM),
        1 << 28,
        (
            pltpu.VMEM((ROWS, COLS), F32),
            pltpu.VMEM((ROWS, COLS), BF16),
            pltpu.VMEM((ROWS, COLS), F32),
            pltpu.VMEM((RANK, COLS), F32),
            pltpu.VMEM((16, 8, LANES), F32),
            pltpu.SemaphoreType.DMA((3, len(READS))),
            pltpu.SemaphoreType.DMA,
        ),
    )(*(pltpu.with_memory_space_constraint(x, HBM) for x in (grads[0], residual[0], q_prev.T)))
    parts = exchange(sent, NEAR)
    incoming = lax.ppermute(outgoing, EVERY, [(a, b) for two in PAIRS for a, b in (two, two[::-1])])
    parts = exchange(call(pass_on, shape(32, 8, LANES), (VMEM,), VMEM, 1 << 15)(parts), FAR)
    left = exchange(call(pass_on, shape(16, 8, LANES), (VMEM,), VMEM, 1 << 15)(parts), NEAR)
    sent = call(share, shape(8, 56, LANES), (VMEM,) * 3, VMEM, 1 << 28)(left, own, incoming)
    first = exchange(sent, ROW)
    second = exchange(call(pass_on, shape(4, 56, LANES), (VMEM,), VMEM, 1 << 17)(first), REST)
    basis, wide, whiten = call(
        factor,
        (shape(RANK, ROWS), shape(ROWS, 3 * RANK, dtype=BF16), shape(RANK, 6 * RANK, dtype=BF16)),
        (VMEM, VMEM),
        (VMEM,) * 3,
        1 << 28,
    )(left, first)
    sent = call(pass_on, shape(16, 56, LANES), (VMEM, VMEM), VMEM, 1 << 17)(second, whiten)
    third = exchange(sent, LINE)
    q_next, new_residual = call(
        finish,
        (HBM((RANK, COLS), F32), HBM((ROWS, COLS), F32)),
        (VMEM,) * 5,
        (HBM, HBM),
        1 << 28,
        (
            pltpu.VMEM((RANK, COLS), F32),
            pltpu.VMEM((3 * RANK, COLS), BF16),
            pltpu.VMEM((ROWS, COLS), F32),
            pltpu.SemaphoreType.DMA((2, len(CUTS))),
        ),
    )(third, wide, whiten, grads[0], residual[0])
    return (q_next.T, basis.T, new_residual[None])


def solution(mesh):
    return jax.shard_map(
        local,
        mesh=mesh,
        in_specs=(P("dp", None, "tensor"), P("dp", None, "tensor"), P("tensor", None)),
        out_specs=(P("tensor", None), P(), P("dp", None, "tensor")),
        check_vma=False,
    )
```

```python
import jax
import jax.numpy as jnp
from jax import lax
from jax.experimental import pallas as pl
from jax.experimental.pallas import tpu as pltpu
from jax.sharding import PartitionSpec as P


EVERY = ("dp", "tensor")
ROWS, RANK, COLS = 256, 64, 1792
N_DP, LANES = 64, 128
HALF = COLS // 2
READS = ((0, 512), (512, 384), (896, 512), (1408, 384))
CUTS = ((0, 512), (512, 512), (1024, 512), (1536, 256))
VMEM, HBM = pltpu.MemorySpace.VMEM, pltpu.MemorySpace.HBM
F32, BF16 = jnp.float32, jnp.bfloat16
NN = (((1,), (0,)), ((), ()))
NT = (((1,), (1,)), ((), ()))


def grouped(key):
    sets = {}
    for z in range(8):
        for y in range(8):
            for t in range(8):
                group, place = key(z, y, t)
                sets.setdefault(group, []).append((place, (z * 8 + y) * 8 + t))
    return [[device for _, device in sorted(members)] for _, members in sorted(sets.items())]


def turned(key):
    return grouped(lambda z, y, t: key(z, y, t) if t % 2 == 1 else key(y, z, t))


NEAR = grouped(lambda z, y, t: ((z, y // 2), (t, y % 2)))
FAR = grouped(lambda z, y, t: ((y % 2, t), (y // 2, z)))
ROW = turned(lambda z, y, t: ((t, y), z))
LINE = turned(lambda z, y, t: ((t, y // 2), (y % 2, z)))
PAIRS = turned(lambda z, y, t: ((t, z, y // 2), y % 2))
REST = turned(lambda z, y, t: ((t, z, y % 2), y // 2))


def exchange(x, groups):
    return lax.all_to_all(x, EVERY, 0, 0, axis_index_groups=groups, tiled=True)


def dot(a, b, dims):
    return lax.dot_general(a, b, dims, preferred_element_type=F32)


def exact(a, b, dims):
    return lax.dot_general(a, b, dims, precision=lax.Precision.HIGHEST, preferred_element_type=F32)


def halves(x):
    high = x.astype(BF16)
    return high, (x - high.astype(F32)).astype(BF16)


def thirds(x):
    high = x.astype(BF16)
    rest = x - high.astype(F32)
    mid = rest.astype(BF16)
    return high, mid, (rest - mid.astype(F32)).astype(BF16)


def kept():
    line = lax.axis_index("dp")
    return jnp.where(lax.axis_index("tensor") % 2 == 1, line % 2, line // 8 % 2)


def half_of(ref, n):
    return ref[:, pl.ds(pl.multiple_of(n * HALF, LANES), HALF)]


def project(grads, residual, right, out, outgoing, own, merged, g_buf, r_buf, q_buf, tiles, sems, sent):
    copies = []
    for n, (start, width) in enumerate(READS):
        at = pl.ds(start, width)
        trio = [
            pltpu.make_async_copy(grads.at[:, at], g_buf.at[:, at], sems.at[0, n]),
            pltpu.make_async_copy(residual.at[:, at], r_buf.at[:, at], sems.at[1, n]),
            pltpu.make_async_copy(right.at[:, at], q_buf.at[:, at], sems.at[2, n]),
        ]
        for copy in trio:
            copy.start()
        copies.append(trio)
    total = jnp.zeros((RANK, ROWS), F32)
    for n, (start, width) in enumerate(READS):
        at = pl.ds(start, width)
        for copy in copies[n]:
            copy.wait()
        m = g_buf[:, at].astype(F32) + r_buf[:, at]
        merged[:, at] = m
        m_high, m_low = halves(m)
        q_high, q_low = halves(q_buf[:, at])
        both = dot(jnp.concatenate([q_high, q_low], axis=0), m_high, NT)
        total += both[:RANK] + both[RANK:] + dot(q_high, m_low, NT)
    for n in range(16):
        i, j = n // 2, n % 2
        tiles[n] = total[8 * i : 8 * i + 8, LANES * j : LANES * (j + 1)]
    copy = pltpu.make_async_copy(tiles, out, sent)
    copy.start()
    outgoing[...] = half_of(merged, 1 - kept())
    own[...] = half_of(merged, kept())
    copy.wait()


def pass_on(parts, *refs):
    out = refs[-1]
    total = parts[0]
    for n in range(1, parts.shape[0]):
        total += parts[n]
    for n in range(out.shape[0]):
        out[n] = total


def left_of(parts):
    left = [jnp.concatenate([parts[2 * i], parts[2 * i + 1]], axis=1) for i in range(8)]
    return jnp.concatenate(left, axis=0) * (1.0 / N_DP)


def place(i, line):
    return 8 * (line // 7) + i, pl.ds(8 * (line % 7), 8)


def share(parts, own, incoming, out):
    high, low = halves(own[...] + incoming[...])
    left_high, left_low = halves(left_of(parts))
    stacked = jnp.concatenate([left_high, left_low], axis=0)
    both = dot(stacked, high, NN)
    mine = both[:RANK] + both[RANK:] + dot(left_high, low, NN)
    for i in range(8):
        for line in range(7):
            out[i, 8 * line : 8 * line + 8, :] = mine[8 * i : 8 * i + 8, LANES * line : LANES * (line + 1)]


def factor(parts, _, basis, wide, whiten):
    left = left_of(parts)
    gram = exact(left, left, NT)
    rows = lax.broadcasted_iota(jnp.int32, (8, LANES), 0)
    row = lax.broadcasted_iota(jnp.int32, (RANK, RANK), 0)
    col = lax.broadcasted_iota(jnp.int32, (RANK, RANK), 1)
    both = jnp.concatenate([jnp.where(row == col, 1.0, 0.0).astype(F32), gram], axis=1)
    v = [both[8 * i : 8 * i + 8] for i in range(8)]
    scaled = []
    for p in range(8):
        b = [
            {i: jnp.broadcast_to(v[i][:, RANK + 8 * p + j : RANK + 8 * p + j + 1], (8, LANES)) for i in range(p, 8)}
            for j in range(8)
        ]
        pivots = b[0][p]
        for k in range(8):
            if k:
                pivots = jnp.where(rows == k, b[k][p], pivots)
            inverse = 1.0 / b[k][p][k : k + 1]
            heads = [b[j][p][k : k + 1] for j in range(8)]
            pivot_row = v[p][k : k + 1]
            for i in range(p, 8):
                c = b[k][i] * inverse
                if i == p:
                    c = jnp.where(rows > k, c, 0.0)
                v[i] = v[i] - c * pivot_row
                for j in range(k + 1, 8):
                    b[j][i] = b[j][i] - c * heads[j]
        scaled.append(v[p] / jnp.sqrt(pivots))
    s = jnp.concatenate(scaled, axis=0)[:, :RANK]
    b_t = exact(s, left, NN)
    basis[...] = b_t
    b_high, b_low = halves(b_t.T)
    wide[...] = jnp.concatenate([b_high, b_high, b_low], axis=1)
    s_high, s_mid, s_low = thirds(s * (1.0 / N_DP))
    whiten[...] = jnp.concatenate([s_high, s_high, s_mid, s_high, s_low, s_mid], axis=1)


def finish(parts, wide, whiten, grads, residual, q_out, out, q_buf, q_cat, o_buf, sems):
    copies = []

    def put(source, target, start, width, sem):
        at = pl.ds(start, width)
        copy = pltpu.make_async_copy(source.at[:, at], target.at[:, at], sem)
        copy.start()
        copies.append(copy)

    for n, (start, width) in enumerate(CUTS):
        columns = []
        for line in range(start // LANES, (start + width) // LANES):
            tiles = []
            for i in range(8):
                sender, rows = place(i, line)
                tiles.append(parts[sender, rows, :])
            columns.append(jnp.concatenate(tiles, axis=0))
        p_high, p_mid, p_low = thirds(jnp.concatenate(columns, axis=1))
        q = dot(whiten[...], jnp.concatenate([p_high, p_mid, p_high, p_low, p_high, p_mid], axis=0), NN)
        q_buf[:, start : start + width] = q
        put(q_buf, q_out, start, width, sems.at[0, n])
        q_high, q_low = halves(q)
        q_cat[:, start : start + width] = jnp.concatenate([q_high, q_low, q_high], axis=0)
    for n, (start, width) in enumerate(CUTS):
        at = slice(start, start + width)
        o_buf[:, at] = grads[:, at].astype(F32) + residual[:, at] - dot(wide[...], q_cat[:, at], NN)
        put(o_buf, out, start, width, sems.at[1, n])
    for copy in copies:
        copy.wait()


def call(kernel, out, ins, outs, flops, scratch=()):
    return pl.pallas_call(
        kernel,
        out_shape=out,
        in_specs=[pl.BlockSpec(memory_space=s) for s in ins],
        out_specs=jax.tree.map(lambda s: pl.BlockSpec(memory_space=s), outs),
        scratch_shapes=list(scratch),
        cost_estimate=pl.CostEstimate(flops=flops, bytes_accessed=1 << 20, transcendentals=0),
        compiler_params=pltpu.CompilerParams(vmem_limit_bytes=16 << 20),
    )


def shape(*dims, dtype=F32):
    return jax.ShapeDtypeStruct(dims, dtype)


def local(grads, residual, q_prev):
    sent, outgoing, own = call(
        project,
        (HBM((16, 8, LANES), F32), shape(ROWS, HALF), shape(ROWS, HALF)),
        (HBM,) * 3,
        (HBM, VMEM, VMEM),
        1 << 28,
        (
            pltpu.VMEM((ROWS, COLS), F32),
            pltpu.VMEM((ROWS, COLS), BF16),
            pltpu.VMEM((ROWS, COLS), F32),
            pltpu.VMEM((RANK, COLS), F32),
            pltpu.VMEM((16, 8, LANES), F32),
            pltpu.SemaphoreType.DMA((3, len(READS))),
            pltpu.SemaphoreType.DMA,
        ),
    )(*(pltpu.with_memory_space_constraint(x, HBM) for x in (grads[0], residual[0], q_prev.T)))
    parts = exchange(sent, NEAR)
    incoming = lax.ppermute(outgoing, EVERY, [(a, b) for two in PAIRS for a, b in (two, two[::-1])])
    parts = exchange(call(pass_on, shape(32, 8, LANES), (VMEM,), VMEM, 1 << 15)(parts), FAR)
    left = exchange(call(pass_on, shape(16, 8, LANES), (VMEM,), VMEM, 1 << 15)(parts), NEAR)
    sent = call(share, shape(8, 56, LANES), (VMEM,) * 3, VMEM, 1 << 28)(left, own, incoming)
    first = exchange(sent, ROW)
    second = exchange(call(pass_on, shape(4, 56, LANES), (VMEM,), VMEM, 1 << 17)(first), REST)
    basis, wide, whiten = call(
        factor,
        (shape(RANK, ROWS), shape(ROWS, 3 * RANK, dtype=BF16), shape(RANK, 6 * RANK, dtype=BF16)),
        (VMEM, VMEM),
        (VMEM,) * 3,
        1 << 28,
    )(left, first)
    sent = call(pass_on, shape(16, 56, LANES), (VMEM, VMEM), VMEM, 1 << 17)(second, whiten)
    third = exchange(sent, LINE)
    q_next, new_residual = call(
        finish,
        (HBM((RANK, COLS), F32), HBM((ROWS, COLS), F32)),
        (VMEM,) * 5,
        (HBM, HBM),
        1 << 28,
        (
            pltpu.VMEM((RANK, COLS), F32),
            pltpu.VMEM((3 * RANK, COLS), BF16),
            pltpu.VMEM((ROWS, COLS), F32),
            pltpu.SemaphoreType.DMA((2, len(CUTS))),
        ),
    )(third, wide, whiten, grads[0], residual[0])
    return (q_next.T, basis.T, new_residual[None])


def solution(mesh):
    return jax.shard_map(
        local,
        mesh=mesh,
        in_specs=(P("dp", None, "tensor"), P("dp", None, "tensor"), P("tensor", None)),
        out_specs=(P("tensor", None), P(), P("dp", None, "tensor")),
        check_vma=False,
    )
```

```python
import jax
import jax.numpy as jnp
from jax import lax
from jax.experimental import pallas as pl
from jax.experimental.pallas import tpu as pltpu
from jax.sharding import PartitionSpec as P


EVERY = ("dp", "tensor")
ROWS, RANK, COLS = 256, 64, 1792
N_DP, LANES = 64, 128
HALF = COLS // 2
READS = ((0, 512), (512, 384), (896, 512), (1408, 384))
CUTS = ((0, 512), (512, 512), (1024, 512), (1536, 256))
VMEM, HBM = pltpu.MemorySpace.VMEM, pltpu.MemorySpace.HBM
F32, BF16 = jnp.float32, jnp.bfloat16
NN = (((1,), (0,)), ((), ()))
NT = (((1,), (1,)), ((), ()))


def grouped(key):
    sets = {}
    for z in range(8):
        for y in range(8):
            for t in range(8):
                group, place = key(z, y, t)
                sets.setdefault(group, []).append((place, (z * 8 + y) * 8 + t))
    return [[device for _, device in sorted(members)] for _, members in sorted(sets.items())]


def turned(key):
    return grouped(lambda z, y, t: key(z, y, t) if t % 2 == 1 else key(y, z, t))


NEAR = grouped(lambda z, y, t: ((z, y // 2), (t, y % 2)))
FAR = grouped(lambda z, y, t: ((y % 2, t), (y // 2, z)))
ROW = turned(lambda z, y, t: ((t, y), z))
LINE = turned(lambda z, y, t: ((t, y // 2), (y % 2, z)))
PAIRS = turned(lambda z, y, t: ((t, z, y // 2), y % 2))
REST = turned(lambda z, y, t: ((t, z, y % 2), y // 2))


def exchange(x, groups):
    return lax.all_to_all(x, EVERY, 0, 0, axis_index_groups=groups, tiled=True)


def dot(a, b, dims):
    return lax.dot_general(a, b, dims, preferred_element_type=F32)


def exact(a, b, dims):
    return lax.dot_general(a, b, dims, precision=lax.Precision.HIGHEST, preferred_element_type=F32)


def halves(x):
    high = x.astype(BF16)
    return high, (x - high.astype(F32)).astype(BF16)


def thirds(x):
    high = x.astype(BF16)
    rest = x - high.astype(F32)
    mid = rest.astype(BF16)
    return high, mid, (rest - mid.astype(F32)).astype(BF16)


def kept():
    line = lax.axis_index("dp")
    return jnp.where(lax.axis_index("tensor") % 2 == 1, line % 2, line // 8 % 2)


def half_of(ref, n):
    return ref[:, pl.ds(pl.multiple_of(n * HALF, LANES), HALF)]


def project(grads, residual, right, out, outgoing, own, merged, g_buf, r_buf, q_buf, tiles, sems, sent):
    copies = []
    for n, (start, width) in enumerate(READS):
        at = pl.ds(start, width)
        trio = [
            pltpu.make_async_copy(residual.at[:, at], r_buf.at[:, at], sems.at[1, n]),
            pltpu.make_async_copy(grads.at[:, at], g_buf.at[:, at], sems.at[0, n]),
            pltpu.make_async_copy(right.at[:, at], q_buf.at[:, at], sems.at[2, n]),
        ]
        for copy in trio:
            copy.start()
        copies.append(trio)
    total = jnp.zeros((RANK, ROWS), F32)
    for n, (start, width) in enumerate(READS):
        at = pl.ds(start, width)
        for copy in copies[n]:
            copy.wait()
        m = g_buf[:, at].astype(F32) + r_buf[:, at]
        merged[:, at] = m
        m_high, m_low = halves(m)
        q_high, q_low = halves(q_buf[:, at])
        both = dot(jnp.concatenate([q_high, q_low], axis=0), m_high, NT)
        total += both[:RANK] + both[RANK:] + dot(q_high, m_low, NT)
    for n in range(16):
        i, j = n // 2, n % 2
        tiles[n] = total[8 * i : 8 * i + 8, LANES * j : LANES * (j + 1)]
    copy = pltpu.make_async_copy(tiles, out, sent)
    copy.start()
    outgoing[...] = half_of(merged, 1 - kept())
    own[...] = half_of(merged, kept())
    copy.wait()


def pass_on(parts, *refs):
    out = refs[-1]
    total = parts[0]
    for n in range(1, parts.shape[0]):
        total += parts[n]
    for n in range(out.shape[0]):
        out[n] = total


def hand_out(parts, out, total, sems):
    acc = parts[0]
    for n in range(1, parts.shape[0]):
        acc += parts[n]
    total[...] = acc
    copies = [pltpu.make_async_copy(total, out.at[n], sems.at[n]) for n in range(4)]
    for copy in copies:
        copy.start()
    for copy in copies:
        copy.wait()


def left_of(parts):
    left = [jnp.concatenate([parts[2 * i], parts[2 * i + 1]], axis=1) for i in range(8)]
    return jnp.concatenate(left, axis=0) * (1.0 / N_DP)


def place(i, line):
    return 8 * (line // 7) + i, pl.ds(8 * (line % 7), 8)


def share(parts, own, incoming, out):
    high, low = halves(own[...] + incoming[...])
    left_high, left_low = halves(left_of(parts))
    stacked = jnp.concatenate([left_high, left_low], axis=0)
    both = dot(stacked, high, NN)
    mine = both[:RANK] + both[RANK:] + dot(left_high, low, NN)
    for i in range(8):
        for line in range(7):
            out[i, 8 * line : 8 * line + 8, :] = mine[8 * i : 8 * i + 8, LANES * line : LANES * (line + 1)]


def factor(parts, _, basis, wide, whiten):
    left = left_of(parts)
    gram = exact(left, left, NT)
    rows = lax.broadcasted_iota(jnp.int32, (8, LANES), 0)
    row = lax.broadcasted_iota(jnp.int32, (RANK, RANK), 0)
    col = lax.broadcasted_iota(jnp.int32, (RANK, RANK), 1)
    both = jnp.concatenate([jnp.where(row == col, 1.0, 0.0).astype(F32), gram], axis=1)
    v = [both[8 * i : 8 * i + 8] for i in range(8)]
    scaled = []
    for p in range(8):
        b = [
            {i: jnp.broadcast_to(v[i][:, RANK + 8 * p + j : RANK + 8 * p + j + 1], (8, LANES)) for i in range(p, 8)}
            for j in range(8)
        ]
        pivots = b[0][p]
        for k in range(8):
            if k:
                pivots = jnp.where(rows == k, b[k][p], pivots)
            inverse = 1.0 / b[k][p][k : k + 1]
            heads = [b[j][p][k : k + 1] for j in range(8)]
            pivot_row = v[p][k : k + 1]
            for i in range(p, 8):
                c = b[k][i] * inverse
                if i == p:
                    c = jnp.where(rows > k, c, 0.0)
                v[i] = v[i] - c * pivot_row
                for j in range(k + 1, 8):
                    b[j][i] = b[j][i] - c * heads[j]
        scaled.append(v[p] / jnp.sqrt(pivots))
    s = jnp.concatenate(scaled, axis=0)[:, :RANK]
    b_t = exact(s, left, NN)
    basis[...] = b_t
    b_high, b_low = halves(b_t.T)
    wide[...] = jnp.concatenate([b_high, b_high, b_low], axis=1)
    s_high, s_mid, s_low = thirds(s * (1.0 / N_DP))
    whiten[...] = jnp.concatenate([s_high, s_high, s_mid, s_high, s_low, s_mid], axis=1)


def finish(parts, wide, whiten, grads, residual, q_out, out, q_buf, q_cat, o_buf, sems):
    copies = []

    def put(source, target, start, width, sem):
        at = pl.ds(start, width)
        copy = pltpu.make_async_copy(source.at[:, at], target.at[:, at], sem)
        copy.start()
        copies.append(copy)

    for n, (start, width) in enumerate(CUTS):
        columns = []
        for line in range(start // LANES, (start + width) // LANES):
            tiles = []
            for i in range(8):
                sender, rows = place(i, line)
                tiles.append(parts[sender, rows, :])
            columns.append(jnp.concatenate(tiles, axis=0))
        p_high, p_mid, p_low = thirds(jnp.concatenate(columns, axis=1))
        q = dot(whiten[...], jnp.concatenate([p_high, p_mid, p_high, p_low, p_high, p_mid], axis=0), NN)
        q_buf[:, start : start + width] = q
        put(q_buf, q_out, start, width, sems.at[0, n])
        q_high, q_low = halves(q)
        q_cat[:, start : start + width] = jnp.concatenate([q_high, q_low, q_high], axis=0)
    for n, (start, width) in enumerate(CUTS):
        at = slice(start, start + width)
        o_buf[:, at] = grads[:, at].astype(F32) + residual[:, at] - dot(wide[...], q_cat[:, at], NN)
        put(o_buf, out, start, width, sems.at[1, n])
    for copy in copies:
        copy.wait()


def call(kernel, out, ins, outs, flops, scratch=()):
    return pl.pallas_call(
        kernel,
        out_shape=out,
        in_specs=[pl.BlockSpec(memory_space=s) for s in ins],
        out_specs=jax.tree.map(lambda s: pl.BlockSpec(memory_space=s), outs),
        scratch_shapes=list(scratch),
        cost_estimate=pl.CostEstimate(flops=flops, bytes_accessed=1 << 20, transcendentals=0),
        compiler_params=pltpu.CompilerParams(vmem_limit_bytes=16 << 20),
    )


def shape(*dims, dtype=F32):
    return jax.ShapeDtypeStruct(dims, dtype)


def local(grads, residual, q_prev):
    sent, outgoing, own = call(
        project,
        (HBM((16, 8, LANES), F32), shape(ROWS, HALF), shape(ROWS, HALF)),
        (HBM,) * 3,
        (HBM, VMEM, VMEM),
        1 << 28,
        (
            pltpu.VMEM((ROWS, COLS), F32),
            pltpu.VMEM((ROWS, COLS), BF16),
            pltpu.VMEM((ROWS, COLS), F32),
            pltpu.VMEM((RANK, COLS), F32),
            pltpu.VMEM((16, 8, LANES), F32),
            pltpu.SemaphoreType.DMA((3, len(READS))),
            pltpu.SemaphoreType.DMA,
        ),
    )(*(pltpu.with_memory_space_constraint(x, HBM) for x in (grads[0], residual[0], q_prev.T)))
    parts = exchange(sent, NEAR)
    incoming = lax.ppermute(outgoing, EVERY, [(a, b) for two in PAIRS for a, b in (two, two[::-1])])
    parts = exchange(call(pass_on, shape(32, 8, LANES), (VMEM,), VMEM, 1 << 15)(parts), FAR)
    left = exchange(call(pass_on, shape(16, 8, LANES), (VMEM,), VMEM, 1 << 15)(parts), NEAR)
    sent = call(share, shape(8, 56, LANES), (VMEM,) * 3, VMEM, 1 << 28)(left, own, incoming)
    first = exchange(sent, ROW)
    sent = call(
        hand_out,
        HBM((4, 56, LANES), F32),
        (VMEM,),
        HBM,
        1 << 17,
        (pltpu.VMEM((56, LANES), F32), pltpu.SemaphoreType.DMA((4,))),
    )(first)
    second = exchange(sent, REST)
    basis, wide, whiten = call(
        factor,
        (shape(RANK, ROWS), shape(ROWS, 3 * RANK, dtype=BF16), shape(RANK, 6 * RANK, dtype=BF16)),
        (VMEM, VMEM),
        (VMEM,) * 3,
        1 << 28,
    )(left, first)
    sent = call(pass_on, shape(16, 56, LANES), (VMEM, VMEM), VMEM, 1 << 17)(second, whiten)
    third = exchange(sent, LINE)
    q_next, new_residual = call(
        finish,
        (HBM((RANK, COLS), F32), HBM((ROWS, COLS), F32)),
        (VMEM,) * 5,
        (HBM, HBM),
        1 << 28,
        (
            pltpu.VMEM((RANK, COLS), F32),
            pltpu.VMEM((3 * RANK, COLS), BF16),
            pltpu.VMEM((ROWS, COLS), F32),
            pltpu.SemaphoreType.DMA((2, len(CUTS))),
        ),
    )(third, wide, whiten, grads[0], residual[0])
    return (q_next.T, basis.T, new_residual[None])


def solution(mesh):
    return jax.shard_map(
        local,
        mesh=mesh,
        in_specs=(P("dp", None, "tensor"), P("dp", None, "tensor"), P("tensor", None)),
        out_specs=(P("tensor", None), P(), P("dp", None, "tensor")),
        check_vma=False,
    )
```
